512 devices in a mesh: segment: 16 (over z_hi, y, core), dp: 32 (over x, z_lo).
Axes of the slice: x: 4, y: 4, z: 16 (z_hi: 2, z_lo: 8; z = z_hi * 8 + z_lo), core: 2. Of those that a mesh axis runs over, the one named last changes fastest.
Arguments:
- token_ids: int32 [4096], P('dp'), may hold values from 0 to 152063, as said below
- table: bfloat16 [19008, 28672], P('segment', 'dp'), may hold values from -6 to 6
- out_grad: bfloat16 [4096, 3584], P('dp', 'segment'), may hold values from -6 to 6
Outputs:
- embedded: bfloat16 [4096, 3584], P('dp')
- table_grad: bfloat16 [19008, 28672], P('segment', 'dp')
The draws below stay inside these ranges and needn't reach their ends.
Inputs may be any that keep to these rules, and one draw needn't show every extreme that they name: `token_ids`: in the 128 tokens of each data group, at most 16 ids lie in one segment's slice of 9504 rows with one residue modulo 8; in every data group some segment and residue has exactly 16.
All inputs are finite; a program needn't handle non-finite values.
Results may differ from the reference program's by a relative error of at most 0.001.
Values may be sent and summed in bfloat16 or wider, within the bound.
A program may use at most 64 MiB of HBM per device.

```python
import jax
import jax.numpy as jnp
from jax import lax

D = 3584
ROWS_SECTION = 9504
PACK = 8
TOK_DEV = 128
VOCAB = 152064
TOKENS = 4096


def draw_token_ids(key, part):
    groups = TOKENS // TOK_DEV
    segments = VOCAB // ROWS_SECTION
    buckets = segments * PACK
    capacity = TOK_DEV // PACK
    lines = ROWS_SECTION // PACK
    global_hot = jax.random.randint(jax.random.fold_in(key, 11), (), 0, buckets)

    def one_group(group):
        group_key = jax.random.fold_in(key, 100 + group)
        keys = jax.random.split(group_key, 7)
        order = jax.random.permutation(keys[0], buckets)
        use_global = jax.random.randint(keys[1], (), 0, 2)
        hot = jnp.where(use_global == 1, global_hot, order[0])
        hot_pos = jnp.argmax(order == hot)
        order = order.at[hot_pos].set(order[0]).at[0].set(hot)
        spread = jax.random.randint(keys[2], (), 7, buckets)
        position = jnp.arange(TOK_DEV)
        bucket = jnp.where(position < capacity, order[0], order[1 + (position - capacity) % spread])
        hot_line = jax.random.randint(keys[3], (TOK_DEV,), 0, min(lines, 4))
        any_line = jax.random.randint(keys[4], (TOK_DEV,), 0, lines)
        pick = jax.random.randint(keys[5], (TOK_DEV,), 0, 2)
        line = jnp.where(pick == 1, hot_line, any_line)
        ids = bucket // PACK * ROWS_SECTION + line * PACK + bucket % PACK
        shuffle = jax.random.permutation(keys[6], TOK_DEV)
        return ids[shuffle]
    return jax.vmap(one_group)(jnp.arange(groups)).reshape(-1).astype(jnp.int32)


def shard_levels(rng, dims, cuts, least, top_value):
    level = 1.0
    for axis_at, shards_of in cuts:
        draws = jax.random.uniform(jax.random.fold_in(jax.random.fold_in(rng, 6), axis_at), (shards_of,), jnp.float32, least / len(cuts), top_value / len(cuts))
        level = level * jnp.repeat(jnp.exp(draws), dims[axis_at] // shards_of).reshape((-1,) + (1,) * (len(dims) - 1 - axis_at))
    return level


def normal_values(own_key, shape, deviation, most, cuts=(), held_as=jnp.bfloat16):
    drawn = jax.random.normal(own_key, shape, jnp.float32) * deviation
    if len(cuts) > 0:
        drawn = shard_levels(own_key, shape, cuts, -0.22, 0.18) * drawn
    return jnp.clip(drawn, min=-most, max=most).astype(held_as)


def setup_inputs(seed: int = 0) -> dict:
    splits = jax.random.split(jax.random.key(seed), 4)
    token_ids = draw_token_ids(jax.random.fold_in(splits[3], 71), 0)
    table = normal_values(splits[1], (VOCAB // PACK, PACK * D), 1.0, 6.0, ((0, 16), (1, 32)))
    out_grad = normal_values(splits[2], (TOKENS, D), 1.0, 6.0, ((0, 32), (1, 16)))
    return {"token_ids": token_ids, "table": table, "out_grad": out_grad}


def reference(token_ids, table, out_grad):
    flat = table.reshape(VOCAB, D)
    embedded = jnp.take(flat, token_ids, axis=0)
    width = 128 if D % 128 == 0 else D
    blocks = D // width
    pieces = out_grad.reshape(TOKENS, blocks, width).transpose(1, 0, 2)

    def accumulate(piece):
        total = jnp.zeros((VOCAB, width), jnp.float32).at[token_ids].add(piece.astype(jnp.float32))
        return total.astype(jnp.bfloat16)

    summed = lax.map(accumulate, pieces)
    table_grad = summed.transpose(1, 0, 2).reshape(VOCAB // PACK, PACK * D)
    return embedded, table_grad
```

```python
import jax
import jax.numpy as jnp
from jax import lax
from jax.experimental import pallas as pl
from jax.experimental.pallas import tpu as pltpu
from jax.sharding import PartitionSpec as P

MESH = pl.DeviceIdType.MESH
D = 3584
PACK = 8
TOK = 128
GROUPS = 32
X, ZL, ZH, YC = 4, 8, 2, 8
Z = ZH * ZL
LINES = 1188
WIDTH = 896
FEATS = 224
BF = jnp.bfloat16


def coords():
    s = lax.axis_index("segment")
    d = lax.axis_index("dp")
    zh = s // YC
    k = s % YC
    x = d // ZL
    zl = d % ZL
    return zh, k, x, zl


def device(z, k, x):
    return ((z // ZL) * YC + k, x * ZL + z % ZL)


def plane_steps():
    return [(dx, dk) for dx in range(X) for dk in range(YC) if dx or dk]


def first_kernel(ids_ref, piece_ref, all_ref, got_ref, local_sem, id_send, id_recv, ft_send, ft_recv):
    zh, k, x, zl = coords()
    z = zh * ZL + zl
    group = x * ZL + zl
    near = [(dx, dz) for dx in range(X) for dz in range(-3, 5) if dx or dz]

    barrier = pltpu.get_barrier_semaphore()
    for dx, dz in near:
        to = device((z + dz + Z) % Z, k, (x + dx) % X)
        pl.semaphore_signal(barrier, inc=1, device_id=to, device_id_type=MESH)
        if dz == 4:
            back = device((z - dz + Z) % Z, k, (x + dx) % X)
            pl.semaphore_signal(barrier, inc=1, device_id=back, device_id_type=MESH)
    for dk in range(1, YC):
        to = device(z, (k + dk) % YC, x)
        pl.semaphore_signal(barrier, inc=1, device_id=to, device_id_type=MESH)
    own_ids = pltpu.make_async_copy(ids_ref.at[0], all_ref.at[group], local_sem.at[0])
    own_ids.start()
    own_piece = pltpu.make_async_copy(piece_ref.at[k], got_ref.at[k], local_sem.at[1])
    own_piece.start()
    pl.semaphore_wait(barrier, len(near) + X + YC - 1)

    copies = []
    for n, (dx, dz) in enumerate(near):
        copy = pltpu.make_async_remote_copy(
            src_ref=ids_ref.at[0],
            dst_ref=all_ref.at[group],
            send_sem=id_send.at[n],
            recv_sem=id_recv.at[n],
            device_id=device((z + dz + Z) % Z, k, (x + dx) % X),
            device_id_type=MESH,
        )
        copy.start()
        copies.append(copy)
    for dk in range(1, YC):
        other = (k + dk) % YC
        copy = pltpu.make_async_remote_copy(
            src_ref=piece_ref.at[other],
            dst_ref=got_ref.at[k],
            send_sem=ft_send.at[dk],
            recv_sem=ft_recv.at[dk],
            device_id=device(z, other, x),
            device_id_type=MESH,
        )
        copy.start()
        copies.append(copy)
    own_ids.wait()
    own_piece.wait()
    for copy in copies:
        copy.wait()


def vmem(n=1):
    return [pl.BlockSpec(memory_space=pltpu.VMEM)] * n


def first_exchange(ids, piece):
    return pl.pallas_call(
        first_kernel,
        out_shape=(
            jax.ShapeDtypeStruct((GROUPS, 1, TOK), jnp.int32),
            jax.ShapeDtypeStruct((YC, 16, FEATS), BF),
        ),
        in_specs=vmem(2),
        out_specs=tuple(vmem(2)),
        scratch_shapes=[
            pltpu.SemaphoreType.DMA((2,)),
            pltpu.SemaphoreType.DMA((GROUPS - 1,)),
            pltpu.SemaphoreType.DMA((GROUPS - 1,)),
            pltpu.SemaphoreType.DMA((YC,)),
            pltpu.SemaphoreType.DMA((YC,)),
        ],
        compiler_params=pltpu.CompilerParams(collective_id=0, has_side_effects=True),
        name="first",
    )(ids, piece)


def onehot(condition):
    return jnp.where(condition, jnp.float32(1), jnp.float32(0)).astype(BF)


def dot(a, b):
    return jnp.dot(a, b, preferred_element_type=jnp.float32).astype(BF)


def main_kernel(
    lcol_ref, lrow_ref, mcol_ref, mrow_ref, pos_ref, table_ref, grad_ref,
    emb_ref, tg_ref,
    es, er, dr, gs, gr, de, zr, fr, fs,
    local_sem, ab_send, ab_recv, zt_send, zt_recv, bt_send, bt_recv, z_send, z_recv, f_send, f_recv,
):
    zh, k, x, zl = coords()
    z = zh * ZL + zl
    me = x * YC + k
    plane = plane_steps()

    barrier = pltpu.get_barrier_semaphore()
    for dx, dk in plane:
        to = device(z, (k + dk) % YC, (x + dx) % X)
        pl.semaphore_signal(barrier, inc=1, device_id=to, device_id_type=MESH)
    for dz in range(1, Z):
        to = device((z + dz) % Z, k, x)
        pl.semaphore_signal(barrier, inc=1, device_id=to, device_id_type=MESH)

    def pick_rows(i, carry):
        rows = pl.ds(pl.multiple_of(i * TOK, TOK), TOK)
        pick = onehot(lcol_ref[rows, :] == lax.broadcasted_iota(jnp.int32, (TOK, LINES), 1))
        es[pl.ds(i * 8, 8)] = dot(pick, table_ref[...]).reshape(8, 16, WIDTH)
        return carry

    lax.fori_loop(0, 4, pick_rows, 0)

    pl.semaphore_wait(barrier, len(plane) + Z - 1)

    def plane_copies(src, dst, send, recv):
        out = []
        for n, (dx, dk) in enumerate(plane):
            ox, ok = (x + dx) % X, (k + dk) % YC
            copy = pltpu.make_async_remote_copy(
                src_ref=src.at[ox * YC + ok],
                dst_ref=dst.at[me],
                send_sem=send.at[n],
                recv_sem=recv.at[n],
                device_id=device(z, ok, ox),
                device_id_type=MESH,
            )
            copy.start()
            out.append(copy)
        return out

    ab = plane_copies(es, er, ab_send, ab_recv)
    own_ab = pltpu.make_async_copy(es.at[me], er.at[me], local_sem.at[0])
    own_ab.start()

    zt = []
    for h in range(2):
        for m in range(4):
            there = 2 * zh + h + 4 * m
            copy = pltpu.make_async_remote_copy(
                src_ref=grad_ref.at[h],
                dst_ref=dr.at[zl],
                send_sem=zt_send.at[h * 4 + m],
                recv_sem=zt_recv.at[zl],
                device_id=device(there, k, x),
                device_id_type=MESH,
            )
            zt.append((there, copy))
            own = pltpu.make_async_copy(grad_ref.at[h], dr.at[zl], local_sem.at[1])

            @pl.when(there != z)
            def _():
                copy.start()

            @pl.when(there == z)
            def _():
                own.start()
                own.wait()

    q = zl % 4
    from_z = (q // 2) * ZL
    for zg in range(ZL):
        @pl.when(from_z + zg != z)
        def _():
            pltpu.make_async_remote_copy(
                src_ref=grad_ref.at[0],
                dst_ref=dr.at[zg],
                send_sem=zt_send.at[0],
                recv_sem=zt_recv.at[zg],
                device_id=device(z, k, x),
                device_id_type=MESH,
            ).wait_recv()

    spread = onehot(
        lax.broadcasted_iota(jnp.int32, (512, TOK), 0) == mrow_ref[...]
    )
    gs[...] = dot(spread, dr[...].reshape(TOK, WIDTH)).reshape(GROUPS, 16, WIDTH)
    bt = plane_copies(gs, gr, bt_send, bt_recv)
    own_bt = pltpu.make_async_copy(gs.at[me], gr.at[me], local_sem.at[2])
    own_bt.start()

    own_ab.wait()
    for copy in ab:
        copy.wait_recv()
    merge = onehot(mcol_ref[...] == lax.broadcasted_iota(jnp.int32, (TOK, 512), 1))
    de[...] = dot(merge, er[...].reshape(512, WIDTH)).reshape(ZL, 16, WIDTH)

    own_z = pltpu.make_async_copy(de.at[zl], zr.at[z], local_sem.at[3])
    own_z.start()
    zc = []
    for dz in range(1, Z):
        there = (z + dz) % Z
        copy = pltpu.make_async_remote_copy(
            src_ref=de.at[there % ZL],
            dst_ref=zr.at[z],
            send_sem=z_send.at[dz],
            recv_sem=z_recv.at[dz],
            device_id=device(there, k, x),
            device_id_type=MESH,
        )
        copy.start()
        zc.append(copy)

    own_bt.wait()
    for copy in bt:
        copy.wait_recv()

    def scatter(start, rows):
        line = start + lax.broadcasted_iota(jnp.int32, (rows, 512), 0)
        place = onehot(line == lrow_ref[...])
        tg_ref[pl.ds(start, rows), :] = dot(place, gr[...].reshape(512, WIDTH))

    def scatter_step(i, carry):
        scatter(pl.multiple_of(i * TOK, TOK), TOK)
        return carry

    lax.fori_loop(0, LINES // TOK, scatter_step, 0)
    scatter(LINES // TOK * TOK, LINES % TOK)

    own_z.wait()
    for copy in zc:
        copy.wait_recv()
    for quarter in range(4):
        total = (
            zr[quarter].astype(jnp.float32)
            + zr[quarter + 4].astype(jnp.float32)
            + zr[quarter + 8].astype(jnp.float32)
            + zr[quarter + 12].astype(jnp.float32)
        )
        fs[:, quarter * WIDTH : (quarter + 1) * WIDTH] = total.astype(BF)

    own_f = pltpu.make_async_copy(fs, fr.at[k], local_sem.at[4])
    own_f.start()
    fc = []
    for dk in range(1, YC):
        copy = pltpu.make_async_remote_copy(
            src_ref=fs,
            dst_ref=fr.at[k],
            send_sem=f_send.at[dk],
            recv_sem=f_recv.at[dk],
            device_id=device(z, (k + dk) % YC, x),
            device_id_type=MESH,
        )
        copy.start()
        fc.append(copy)
    own_f.wait()
    for copy in fc:
        copy.wait_recv()
    back = onehot(pos_ref[...] == lax.broadcasted_iota(jnp.int32, (TOK, TOK), 1))
    emb_ref[...] = dot(back, fr[...].reshape(TOK, D))

    for copy in ab + bt + zc + fc:
        copy.wait_send()
    for there, copy in zt:
        @pl.when(there != z)
        def _():
            copy.wait_send()


def main_exchange(lcol, lrow, mcol, mrow, pos, table, grad):
    dma = pltpu.SemaphoreType.DMA
    return pl.pallas_call(
        main_kernel,
        out_shape=(
            jax.ShapeDtypeStruct((TOK, D), BF),
            jax.ShapeDtypeStruct((LINES, WIDTH), BF),
        ),
        in_specs=vmem(7),
        out_specs=tuple(vmem(2)),
        scratch_shapes=[
            pltpu.VMEM((GROUPS, 16, WIDTH), BF),
            pltpu.VMEM((GROUPS, 16, WIDTH), BF),
            pltpu.VMEM((ZL, 16, WIDTH), BF),
            pltpu.VMEM((GROUPS, 16, WIDTH), BF),
            pltpu.VMEM((GROUPS, 16, WIDTH), BF),
            pltpu.VMEM((ZL, 16, WIDTH), BF),
            pltpu.VMEM((Z, 16, WIDTH), BF),
            pltpu.VMEM((YC, 16, D), BF),
            pltpu.VMEM((16, D), BF),
            dma((5,)),
            dma((31,)), dma((31,)),
            dma((8,)), dma((8,)),
            dma((31,)), dma((31,)),
            dma((16,)), dma((16,)),
            dma((8,)), dma((8,)),
        ],
        compiler_params=pltpu.CompilerParams(
            collective_id=1, has_side_effects=True, vmem_limit_bytes=48 * 1024 * 1024
        ),
        name="main",
    )(lcol, lrow, mcol, mrow, pos, table, grad)


def sorted_places(ids):
    bucket = ids // (LINES * PACK) * PACK + ids % PACK
    at = jnp.arange(TOK, dtype=jnp.int32)
    key = bucket * TOK + at
    less = key[:, None, :] < key[:, :, None]
    same = bucket[:, None, :] == bucket[:, :, None]
    place = jnp.sum(less.astype(jnp.int32), axis=2)
    rank = jnp.sum((less & same).astype(jnp.int32), axis=2)
    return bucket, place, rank


def body(token_ids, table, out_grad):
    zh, k, x, zl = coords()
    parity = zl // 4
    steps16 = jnp.arange(16, dtype=jnp.int32)

    _, own_place, _ = sorted_places(token_ids[None])
    own_place = own_place[0]
    pos = own_place % 8 * 16 + own_place // 8
    order = onehot(jnp.arange(TOK, dtype=jnp.int32)[:, None] == pos[None, :])
    piece = dot(order, out_grad).reshape(YC, 16, FEATS)

    all_ids, got = first_exchange(token_ids.reshape(1, 1, TOK), piece)
    grad = got.reshape(2, 4, 16, FEATS).transpose(0, 2, 1, 3).reshape(2, 16, WIDTH)

    ids = all_ids.reshape(GROUPS, TOK)
    bucket, place, rank = sorted_places(ids)
    line = ids % (LINES * PACK) // PACK
    slot = 2 * x + parity
    mine = bucket == (zh * YC + k) * PACK + slot
    code = jnp.where(mine, place % 8 * 2 + rank // 8, -1)
    found = jnp.sum(
        jnp.where(code[:, None, :] == steps16[None, :, None], line[:, None, :] + 1, 0), axis=2
    ) - 1
    wanted = found.reshape(X, ZL, YC, 2).transpose(0, 2, 1, 3).reshape(512)

    def of_mine(a):
        return lax.dynamic_slice_in_dim(a, x * ZL, ZL, 0)

    near_bucket, near_place, near_rank = of_mine(bucket), of_mine(place), of_mine(rank)
    segment, owner_slot = near_bucket // PACK, near_bucket % PACK
    here = (segment // YC == zh) & (owner_slot % 2 == parity)
    source = (owner_slot // 2 * YC + segment % YC) * 16 + near_rank // 8
    source = source + 2 * jnp.arange(ZL, dtype=jnp.int32)[:, None]
    value = jnp.where(here, source + 1, 0)
    at = near_place[:, None, :] == (steps16 * 8 + k)[None, :, None]
    merged = (jnp.sum(jnp.where(at, value[:, None, :], 0), axis=2) - 1).reshape(TOK)

    return main_exchange(
        wanted[:, None], wanted[None, :], merged[:, None], merged[None, :], pos[:, None], table, grad
    )


def solution(mesh):
    return jax.shard_map(
        body,
        mesh=mesh,
        in_specs=(P("dp"), P("segment", "dp"), P("dp", "segment")),
        out_specs=(P("dp", None), P("segment", "dp")),
        check_vma=False,
    )
```

```python
import jax
import jax.numpy as jnp
from jax import lax
from jax.experimental import pallas as pl
from jax.experimental.pallas import tpu as pltpu
from jax.sharding import PartitionSpec as P

MESH = pl.DeviceIdType.MESH
D = 3584
PACK = 8
TOK = 128
GROUPS = 32
X, ZL, ZH, YC = 4, 8, 2, 8
Z = ZH * ZL
LINES = 1188
WIDTH = 896
FEATS = 224
BF = jnp.bfloat16
F32 = jnp.float32
CUTS = (256, 384, 256)
STARTS = (0, 256, 640)


def coords():
    s = lax.axis_index("segment")
    d = lax.axis_index("dp")
    zh = s // YC
    k = s % YC
    x = d // ZL
    zl = d % ZL
    return zh, k, x, zl


def device(z, k, x):
    return ((z // ZL) * YC + k, x * ZL + z % ZL)


def plane_steps():
    return [(dx, dk) for dx in range(X) for dk in range(YC) if dx or dk]


def vmem(n=1):
    return [pl.BlockSpec(memory_space=pltpu.VMEM)] * n


def onehot(condition):
    return jnp.where(condition, F32(1), F32(0)).astype(BF)


def dot(a, b):
    return jnp.dot(a, b, preferred_element_type=F32).astype(BF)


def iota(shape, dim):
    return lax.broadcasted_iota(jnp.int32, shape, dim).astype(F32)


def remote(src, dst, send, recv, to):
    copy = pltpu.make_async_remote_copy(
        src_ref=src, dst_ref=dst, send_sem=send, recv_sem=recv, device_id=to, device_id_type=MESH
    )
    copy.start()
    return copy


def local(src, dst, sem):
    copy = pltpu.make_async_copy(src, dst, sem)
    copy.start()
    return copy


def settle(ref, sem):
    pltpu.make_async_copy(ref, ref, sem).wait()


def whole_kernel(
    ids_ref, table_hbm, gradt_ref, emb_ref, tg_ref,
    table, info, mine, piece, got, place_at, gq, order_ref, s_ref, lrow_ref,
    es0, es1, es2, er0, er1, er2, dr, gs, gr, de0, de1, de2, zr0, zr1, zr2,
    fs0, fs1, fs2, fr0, fr1, fr2,
    table_sem, id_send, id_recv, ft_send, ft_recv, zt_send, zt_recv,
    ab_send, ab_recv, bt_send, bt_recv, z_send, z_recv, f_send, f_recv,
):
    es, er, de, zr = (es0, es1, es2), (er0, er1, er2), (de0, de1, de2), (zr0, zr1, zr2)
    fs, fr = (fs0, fs1, fs2), (fr0, fr1, fr2)
    zh, k, x, zl = coords()
    z = zh * ZL + zl
    me = x * YC + k
    group = x * ZL + zl
    parity = zl // 4
    plane = plane_steps()
    near = [(dx, dz) for dx in range(X) for dz in range(-4, 5) if dz]

    barrier = pltpu.get_barrier_semaphore()
    for dx, dz in near:
        to = device((z + dz + Z) % Z, k, (x + dx) % X)
        pl.semaphore_signal(barrier, inc=1, device_id=to, device_id_type=MESH)
    for dx, dk in plane:
        to = device(z, (k + dk) % YC, (x + dx) % X)
        pl.semaphore_signal(barrier, inc=1, device_id=to, device_id_type=MESH)
    table_copy = local(table_hbm, table, table_sem)

    ids = ids_ref[...]
    segment = ((ids.astype(F32) + 0.5) * F32(1.0 / (LINES * PACK))).astype(jnp.int32)
    slot = ids & 7
    line = (ids - segment * (LINES * PACK)) >> 3
    bucket = segment * PACK + slot
    key = (bucket * TOK + lax.broadcasted_iota(jnp.int32, (1, TOK), 1)).astype(F32)
    keys = jnp.broadcast_to(key, (TOK, TOK))
    turned = keys.T
    first = (bucket * TOK).astype(F32)
    at = jnp.sum(jnp.where(turned < keys, F32(1), F32(0)), axis=0, keepdims=True)
    begin = jnp.sum(jnp.where(turned < first, F32(1), F32(0)), axis=0, keepdims=True)
    at = at.astype(jnp.int32)
    second = (at - begin.astype(jnp.int32)) >> 3
    klass, inside = at & 7, at >> 3
    rows = (
        line + 1,
        bucket,
        klass * 16 + second,
        klass,
        inside,
        ((slot >> 1) * YC + (segment & 7)) * 16 + second,
        (segment >> 3) * 2 + (slot & 1),
        slot,
    )
    for n, row in enumerate(rows):
        mine[n : n + 1, :] = row.astype(F32)
    order = jnp.where(
        iota((TOK, TOK), 0) == (klass * 16 + inside).astype(F32), F32(1), F32(0)
    )
    order_ref[...] = order.T.astype(BF)
    sorted_grad = lax.dot_general(
        order.astype(BF), gradt_ref[...], (((1,), (1,)), ((), ())), preferred_element_type=F32
    ).astype(BF)
    piece[...] = sorted_grad.reshape(YC, 16, FEATS)
    for j in range(4):
        place_at[j] = onehot(iota((FEATS, WIDTH), 0) + F32(FEATS * j) == iota((FEATS, WIDTH), 1))

    pl.semaphore_wait(barrier, len(near) + len(plane))

    for dx, dz in [(dx, dz) for dx in range(X) for dz in range(-3, 5) if dx or dz]:
        remote(mine, info.at[group], id_send, id_recv, device((z + dz + Z) % Z, k, (x + dx) % X))
    local(mine, info.at[group], id_recv)
    for dk in range(1, YC):
        other = (k + dk) % YC
        remote(piece.at[other], got.at[k], ft_send, ft_recv, device(z, other, x))
    local(piece.at[k], got.at[k], ft_recv)

    settle(got, ft_recv)
    for h in range(2):
        total = jnp.zeros((16, WIDTH), F32)
        for j in range(4):
            total = total + jnp.dot(got[4 * h + j], place_at[j], preferred_element_type=F32)
        gq[h] = total.astype(BF)
    settle(info, id_recv)

    zt = []
    for h in range(2):
        for m in range(4):
            there = 2 * zh + h + 4 * m
            copy = pltpu.make_async_remote_copy(
                src_ref=gq.at[h],
                dst_ref=dr.at[zl],
                send_sem=zt_send.at[h * 4 + m],
                recv_sem=zt_recv,
                device_id=device(there, k, x),
                device_id_type=MESH,
            )
            zt.append((there, copy))

            @pl.when(there != z)
            def _():
                copy.start()

            @pl.when(there == z)
            def _():
                local(gq.at[h], dr.at[zl], zt_recv)

    sub = iota((TOK, TOK), 0)
    my_bucket = ((zh * YC + k) * PACK + 2 * x + parity).astype(F32)
    for ox in range(X):
        acc = jnp.zeros((TOK, TOK), F32)
        for zg in range(ZL):
            rows = info[ox * ZL + zg]
            code = jnp.where(rows[1:2] == my_bucket, rows[2:3] + F32(2 * zg), F32(-1))
            acc = acc + jnp.where(sub == code, rows[0:1], F32(0))
        lcol = jnp.sum(acc, axis=1, keepdims=True) - 1
        lrow_ref[:, ox * TOK : (ox + 1) * TOK] = jnp.sum(acc.T, axis=0, keepdims=True) - 1
        s_ref[ox * TOK : (ox + 1) * TOK, :] = onehot(lcol == iota((TOK, LINES), 1))
    table_copy.wait()

    def plane_copies(src, dst, send, recv):
        for dx, dk in plane:
            ox, ok = (x + dx) % X, (k + dk) % YC
            remote(src.at[ox * YC + ok], dst.at[me], send, recv, device(z, ok, ox))
        local(src.at[me], dst.at[me], recv)

    for c, (start, width) in enumerate(zip(STARTS, CUTS)):
        def pick_rows(i, carry):
            rows = pl.ds(pl.multiple_of(i * TOK, TOK), TOK)
            picked = dot(s_ref[rows, :], table[:, start : start + width])
            es[c][pl.ds(i * 8, 8)] = picked.reshape(8, 16, width)
            return carry

        lax.fori_loop(0, 4, pick_rows, 0)
        plane_copies(es[c], er[c], ab_send.at[c], ab_recv.at[c])

    acc = jnp.zeros((TOK, TOK), F32)
    my_half = (zh * 2 + parity).astype(F32)
    my_class = k.astype(F32)
    for zg in range(ZL):
        rows = info[x * ZL + zg]
        here = (rows[3:4] == my_class) & (rows[6:7] == my_half)
        code = jnp.where(here, rows[4:5] + F32(16 * zg), F32(-1))
        acc = acc + jnp.where(sub == code, rows[5:6] + F32(2 * zg + 1), F32(0))
    mcol = jnp.sum(acc, axis=1, keepdims=True) - 1
    mrow = jnp.sum(acc.T, axis=0, keepdims=True) - 1
    merge = onehot(mcol == iota((TOK, 512), 1))
    spread = onehot(iota((512, TOK), 0) == mrow)

    def merge_and_send(c):
        settle(er[c], ab_recv.at[c])
        de[c][...] = dot(merge, er[c][...].reshape(512, CUTS[c])).reshape(ZL, 16, CUTS[c])
        for dz in range(1, Z):
            there = (z + dz) % Z
            remote(de[c].at[there % ZL], zr[c].at[z], z_send.at[c], z_recv.at[c], device(there, k, x))
        local(de[c].at[zl], zr[c].at[z], z_recv.at[c])

    merge_and_send(0)
    settle(dr, zt_recv)
    gs[...] = dot(spread, dr[...].reshape(TOK, WIDTH)).reshape(GROUPS, 16, WIDTH)
    merge_and_send(1)
    plane_copies(gs, gr, bt_send, bt_recv)
    merge_and_send(2)

    def sum_and_send(c):
        settle(zr[c], z_recv.at[c])
        for quarter in range(4):
            total = zr[c][quarter].astype(F32)
            for m in range(1, 4):
                total = total + zr[c][quarter + 4 * m].astype(F32)
            fs[c][quarter] = total.astype(BF)
        for dk in range(1, YC):
            remote(fs[c], fr[c].at[k], f_send.at[c], f_recv.at[c], device(z, (k + dk) % YC, x))
        local(fs[c], fr[c].at[k], f_recv.at[c])

    def finish(c):
        settle(fr[c], f_recv.at[c])
        for quarter in range(4):
            start = quarter * WIDTH + STARTS[c]
            rows = fr[c][:, quarter].reshape(TOK, CUTS[c])
            emb_ref[:, start : start + CUTS[c]] = dot(order_ref[...], rows)

    sum_and_send(0)
    sum_and_send(1)
    settle(gr, bt_recv)

    def scatter(start, rows):
        line = (start + lax.broadcasted_iota(jnp.int32, (rows, 512), 0)).astype(F32)
        place = onehot(line == lrow_ref[...])
        tg_ref[pl.ds(start, rows), :] = dot(place, gr[...].reshape(512, WIDTH))

    def scatter_step(i, carry):
        scatter(pl.multiple_of(i * TOK, TOK), TOK)
        return carry

    lax.fori_loop(0, LINES // TOK, scatter_step, 0)
    scatter(LINES // TOK * TOK, LINES % TOK)
    finish(0)
    sum_and_send(2)
    finish(1)
    finish(2)

    settle(info.at[pl.ds(0, GROUPS - 1)], id_send)
    settle(got.at[pl.ds(0, YC - 1)], ft_send)
    settle(gr.at[pl.ds(0, GROUPS - 1)], bt_send)
    for c in range(3):
        settle(er[c].at[pl.ds(0, GROUPS - 1)], ab_send.at[c])
        settle(zr[c].at[pl.ds(0, Z - 1)], z_send.at[c])
        settle(fr[c].at[pl.ds(0, YC - 1)], f_send.at[c])
    for there, copy in zt:
        @pl.when(there != z)
        def _():
            copy.wait_send()


def body(token_ids, table, out_grad):
    dma = pltpu.SemaphoreType.DMA

    def each(*lead):
        return [pltpu.VMEM((*lead, width), BF) for width in CUTS]

    return pl.pallas_call(
        whole_kernel,
        out_shape=(
            jax.ShapeDtypeStruct((TOK, D), BF),
            jax.ShapeDtypeStruct((LINES, WIDTH), BF),
        ),
        in_specs=[vmem()[0], pl.BlockSpec(memory_space=pl.ANY), vmem()[0]],
        out_specs=tuple(vmem(2)),
        scratch_shapes=[
            pltpu.VMEM((LINES, WIDTH), BF),
            pltpu.VMEM((GROUPS, 8, TOK), F32),
            pltpu.VMEM((8, TOK), F32),
            pltpu.VMEM((YC, 16, FEATS), BF),
            pltpu.VMEM((YC, 16, FEATS), BF),
            pltpu.VMEM((4, FEATS, WIDTH), BF),
            pltpu.VMEM((2, 16, WIDTH), BF),
            pltpu.VMEM((TOK, TOK), BF),
            pltpu.VMEM((512, LINES), BF),
            pltpu.VMEM((1, 512), F32),
            *each(GROUPS, 16),
            *each(GROUPS, 16),
            pltpu.VMEM((ZL, 16, WIDTH), BF),
            pltpu.VMEM((GROUPS, 16, WIDTH), BF),
            pltpu.VMEM((GROUPS, 16, WIDTH), BF),
            *each(ZL, 16),
            *each(Z, 16),
            *each(4, 16),
            *each(YC, 4, 16),
            dma, dma, dma, dma, dma, dma((8,)), dma,
            dma((3,)), dma((3,)), dma, dma, dma((3,)), dma((3,)), dma((3,)), dma((3,)),
        ],
        compiler_params=pltpu.CompilerParams(
            collective_id=0, has_side_effects=True, vmem_limit_bytes=48 * 1024 * 1024
        ),
        name="whole",
    )(token_ids.reshape(1, TOK), table, out_grad.T)


def solution(mesh):
    return jax.shard_map(
        body,
        mesh=mesh,
        in_specs=(P("dp"), P("segment", "dp"), P("dp", "segment")),
        out_specs=(P("dp", None), P("segment", "dp")),
        check_vma=False,
    )
```

```python
import jax
import jax.numpy as jnp
from jax import lax
from jax.experimental import pallas as pl
from jax.experimental.pallas import tpu as pltpu
from jax.sharding import PartitionSpec as P

MESH = pl.DeviceIdType.MESH
D = 3584
PACK = 8
TOK = 128
GROUPS = 32
X, ZL, ZH, YC = 4, 8, 2, 8
Z = ZH * ZL
LINES = 1188
WIDTH = 896
FEATS = 224
BF = jnp.bfloat16
F32 = jnp.float32
CUTS = (256, 256, 256, 128)
STARTS = (0, 256, 512, 768)
N = len(CUTS)


def coords():
    s = lax.axis_index("segment")
    d = lax.axis_index("dp")
    zh = s // YC
    k = s % YC
    x = d // ZL
    zl = d % ZL
    return zh, k, x, zl


def device(z, k, x):
    return ((z // ZL) * YC + k, x * ZL + z % ZL)


def plane_steps():
    return [(dx, dk) for dx in range(X) for dk in range(YC) if dx or dk]


def onehot(condition):
    return jnp.where(condition, F32(1), F32(0)).astype(BF)


def dot(a, b):
    return jnp.dot(a, b, preferred_element_type=F32).astype(BF)


def iota(shape, dim):
    return lax.broadcasted_iota(jnp.int32, shape, dim).astype(F32)


def remote(src, dst, send, recv, to):
    copy = pltpu.make_async_remote_copy(
        src_ref=src, dst_ref=dst, send_sem=send, recv_sem=recv, device_id=to, device_id_type=MESH
    )
    copy.start()
    return copy


def local(src, dst, sem):
    copy = pltpu.make_async_copy(src, dst, sem)
    copy.start()
    return copy


def settle(ref, sem):
    pltpu.make_async_copy(ref, ref, sem).wait()


def whole_kernel(
    ids_hbm, table_hbm, gradt_hbm, emb_hbm, tg_hbm,
    emb_ref, tg_ref, ids_ref, gradt_ref, table, info, flat, rt_ref, val_ref, mine, piece, got, place_at, gq, order_ref,
    s_ref, lrow_ref, dr, gs, gr, *rest,
):
    es, er, de, zr, fs, fr, held = (rest[n * N : (n + 1) * N] for n in range(7))
    (
        in_sem, id_send, id_recv, ft_send, ft_recv, zt_send, zt_recv, bt_send, bt_recv,
        ab_send, ab_recv, z_send, z_recv, f_send, f_recv, h_recv, h_send, out_sem, tg_sem,
    ) = rest[7 * N :]
    zh, k, x, zl = coords()
    z = zh * ZL + zl
    me = x * YC + k
    group = x * ZL + zl
    parity = zl // 4
    plane = plane_steps()
    near = [(dx, dz) for dx in range(X) for dz in range(-4, 5) if dz]

    barrier = pltpu.get_barrier_semaphore()
    for dx, dz in near:
        to = device((z + dz + Z) % Z, k, (x + dx) % X)
        pl.semaphore_signal(barrier, inc=1, device_id=to, device_id_type=MESH)
    for dx, dk in plane:
        to = device(z, (k + dk) % YC, (x + dx) % X)
        pl.semaphore_signal(barrier, inc=1, device_id=to, device_id_type=MESH)
    ids_copy = local(ids_hbm, ids_ref, in_sem.at[0])
    grad_copy = local(gradt_hbm, gradt_ref, in_sem.at[1])
    table_copy = local(table_hbm, table, in_sem.at[2])

    ids_copy.wait()
    ids = ids_ref[...]
    segment = ((ids.astype(F32) + 0.5) * F32(1.0 / (LINES * PACK))).astype(jnp.int32)
    slot = ids & 7
    key = ((segment * PACK + slot) * TOK + lax.broadcasted_iota(jnp.int32, (1, TOK), 1)).astype(F32)
    keys = jnp.broadcast_to(key, (TOK, TOK))
    at = jnp.sum(jnp.where(keys.T < keys, F32(1), F32(0)), axis=0, keepdims=True)
    mine[:, :TOK] = ids.astype(F32)
    mine[:, TOK:] = at
    at = at.astype(jnp.int32)
    klass, inside = at & 7, at >> 3
    order = jnp.where(
        iota((TOK, TOK), 0) == (klass * 16 + inside).astype(F32), F32(1), F32(0)
    )
    order_ref[...] = order.T.astype(BF)
    grad_copy.wait()
    sorted_grad = lax.dot_general(
        order.astype(BF), gradt_ref[...], (((1,), (1,)), ((), ())), preferred_element_type=F32
    ).astype(BF)
    piece[...] = sorted_grad.reshape(YC, 16, FEATS)
    for j in range(4):
        place_at[j] = onehot(iota((FEATS, WIDTH), 0) + F32(FEATS * j) == iota((FEATS, WIDTH), 1))

    pl.semaphore_wait(barrier, len(near) + len(plane))

    for dx, dz in [(dx, dz) for dx in range(X) for dz in range(-3, 5) if dx or dz]:
        remote(mine, info.at[group], id_send, id_recv, device((z + dz + Z) % Z, k, (x + dx) % X))
    local(mine, info.at[group], id_recv)
    for dk in range(1, YC):
        other = (k + dk) % YC
        remote(piece.at[other], got.at[k], ft_send, ft_recv, device(z, other, x))
    local(piece.at[k], got.at[k], ft_recv)

    settle(got, ft_recv)
    for h in range(2):
        total = jnp.zeros((16, WIDTH), F32)
        for j in range(4):
            total = total + jnp.dot(got[4 * h + j], place_at[j], preferred_element_type=F32)
        gq[h] = total.astype(BF)
    settle(info, id_recv)

    zt = []
    for h in range(2):
        for m in range(4):
            there = 2 * zh + h + 4 * m
            copy = pltpu.make_async_remote_copy(
                src_ref=gq.at[h],
                dst_ref=dr.at[zl],
                send_sem=zt_send.at[h * 4 + m],
                recv_sem=zt_recv,
                device_id=device(there, k, x),
                device_id_type=MESH,
            )
            zt.append((there, copy))

            @pl.when(there != z)
            def _():
                copy.start()

            @pl.when(there == z)
            def _():
                local(gq.at[h], dr.at[zl], zt_recv)

    for g in range(GROUPS):
        flat[g : g + 1, :] = info[g]
    ids = flat[:, :TOK]
    segment = ((ids + 0.5) * F32(1.0 / (LINES * PACK))).astype(jnp.int32)
    ids = ids.astype(jnp.int32)
    slot = ids & 7
    line = (ids - segment * (LINES * PACK)) >> 3
    at = flat[:, TOK:].astype(jnp.int32)
    klass, inside = at & 7, at >> 3
    second = inside & 1
    zg_row = lax.broadcasted_iota(jnp.int32, (GROUPS, TOK), 0) & 7
    my_bucket = (zh * YC + k) * PACK + 2 * x + parity
    code = jnp.where(segment * PACK + slot == my_bucket, klass * 16 + second + 2 * zg_row, -1).astype(F32)
    line = (line + 1).astype(F32)
    here = (klass == k) & (segment >> 3 == zh) & (slot & 1 == parity)
    rt_ref[...] = jnp.where(here, inside + 16 * zg_row, -1).astype(F32)
    source = ((slot >> 1) * YC + (segment & 7)) * 16 + second
    val_ref[...] = (source + 2 * zg_row + 1).astype(F32)

    sub = iota((TOK, TOK), 0)
    for ox in range(X):
        acc = jnp.zeros((TOK, TOK), F32)
        for g in range(ox * ZL, (ox + 1) * ZL):
            acc = acc + jnp.where(sub == code[g : g + 1], line[g : g + 1], F32(0))
        lcol = jnp.sum(acc, axis=1, keepdims=True) - 1
        lrow_ref[:, ox * TOK : (ox + 1) * TOK] = jnp.sum(acc.T, axis=0, keepdims=True) - 1
        s_ref[ox * TOK : (ox + 1) * TOK, :] = onehot(lcol == iota((TOK, LINES), 1))
    table_copy.wait()

    def plane_copies(src, dst, send, recv):
        for dx, dk in plane:
            ox, ok = (x + dx) % X, (k + dk) % YC
            remote(src.at[ox * YC + ok], dst.at[me], send, recv, device(z, ok, ox))
        local(src.at[me], dst.at[me], recv)

    for c, (start, width) in enumerate(zip(STARTS, CUTS)):
        def pick_rows(i, carry):
            rows = pl.ds(pl.multiple_of(i * TOK, TOK), TOK)
            picked = dot(s_ref[rows, :], table[:, start : start + width])
            es[c][pl.ds(i * 8, 8)] = picked.reshape(8, 16, width)
            return carry

        lax.fori_loop(0, 4, pick_rows, 0)
        plane_copies(es[c], er[c], ab_send.at[c], ab_recv.at[c])

    acc = jnp.zeros((TOK, TOK), F32)
    own = pl.ds(pl.multiple_of(x * ZL, ZL), ZL)
    rt, val = rt_ref[own, :], val_ref[own, :]
    for zg in range(ZL):
        acc = acc + jnp.where(sub == rt[zg : zg + 1], val[zg : zg + 1], F32(0))
    mcol = jnp.sum(acc, axis=1, keepdims=True) - 1
    mrow = jnp.sum(acc.T, axis=0, keepdims=True) - 1
    merge = onehot(mcol == iota((TOK, 512), 1))
    spread = onehot(iota((512, TOK), 0) == mrow)

    def merge_and_send(c):
        settle(er[c], ab_recv.at[c])
        de[c][...] = dot(merge, er[c][...].reshape(512, CUTS[c])).reshape(ZL, 16, CUTS[c])
        opposite = (z + 8) % Z
        low, high = pl.ds(0, 8), pl.ds(8, 8)
        remote(de[c].at[opposite % ZL, high], held[c], z_send.at[c], h_recv.at[c], device((z + 12) % Z, k, x))
        remote(de[c].at[opposite % ZL, low], zr[c].at[z, low], z_send.at[c], z_recv.at[c], device(opposite, k, x))
        for dz in (9, 7, 10, 6, 11, 5, 12, 4, 13, 3, 14, 2, 15, 1):
            there = (z + dz) % Z
            remote(de[c].at[there % ZL], zr[c].at[z], z_send.at[c], z_recv.at[c], device(there, k, x))
        local(de[c].at[zl], zr[c].at[z], z_recv.at[c])

    def pass_on(c):
        settle(held[c], h_recv.at[c])
        behind = device((z + 12) % Z, k, x)
        remote(held[c], zr[c].at[(z + 4) % Z, pl.ds(8, 8)], h_send.at[c], z_recv.at[c], behind)

    merge_and_send(0)
    settle(dr, zt_recv)
    gs[...] = dot(spread, dr[...].reshape(TOK, WIDTH)).reshape(GROUPS, 16, WIDTH)
    merge_and_send(1)
    plane_copies(gs, gr, bt_send, bt_recv)
    pass_on(0)
    merge_and_send(2)
    pass_on(1)
    merge_and_send(3)

    def sum_and_send(c):
        settle(zr[c], z_recv.at[c])
        for quarter in range(4):
            total = zr[c][quarter].astype(F32)
            for m in range(1, 4):
                total = total + zr[c][quarter + 4 * m].astype(F32)
            fs[c][quarter] = total.astype(BF)
        for dk in range(1, YC):
            remote(fs[c], fr[c].at[k], f_send.at[c], f_recv.at[c], device(z, (k + dk) % YC, x))
        local(fs[c], fr[c].at[k], f_recv.at[c])

    def finish(c):
        settle(fr[c], f_recv.at[c])
        for quarter in range(4):
            start = quarter * WIDTH + STARTS[c]
            rows = fr[c][:, quarter].reshape(TOK, CUTS[c])
            columns = slice(start, start + CUTS[c])
            emb_ref[:, columns] = dot(order_ref[...], rows)
            local(emb_ref.at[:, columns], emb_hbm.at[:, columns], out_sem.at[c])

    sum_and_send(0)
    pass_on(2)
    sum_and_send(1)
    pass_on(3)
    settle(gr, bt_recv)

    def scatter(start, rows):
        line = (start + lax.broadcasted_iota(jnp.int32, (rows, 512), 0)).astype(F32)
        place = onehot(line == lrow_ref[...])
        tg_ref[pl.ds(start, rows), :] = dot(place, gr[...].reshape(512, WIDTH))

    def scatter_step(i, carry):
        scatter(pl.multiple_of(i * TOK, TOK), TOK)
        return carry

    lax.fori_loop(0, LINES // TOK, scatter_step, 0)
    scatter(LINES // TOK * TOK, LINES % TOK)
    local(tg_ref, tg_hbm, tg_sem)
    finish(0)
    sum_and_send(2)
    finish(1)
    sum_and_send(3)
    finish(2)
    finish(3)

    settle(info.at[pl.ds(0, GROUPS - 1)], id_send)
    settle(tg_ref, tg_sem)
    settle(got.at[pl.ds(0, YC - 1)], ft_send)
    settle(gr.at[pl.ds(0, GROUPS - 1)], bt_send)
    for c in range(N):
        settle(held[c], h_send.at[c])
        settle(emb_ref.at[:, : 4 * CUTS[c]], out_sem.at[c])
        settle(er[c].at[pl.ds(0, GROUPS - 1)], ab_send.at[c])
        settle(zr[c].at[pl.ds(0, Z - 1)], z_send.at[c])
        settle(fr[c].at[pl.ds(0, YC - 1)], f_send.at[c])
    for there, copy in zt:
        @pl.when(there != z)
        def _():
            copy.wait_send()


def body(token_ids, table, out_grad):
    dma = pltpu.SemaphoreType.DMA

    def each(*lead):
        return [pltpu.VMEM((*lead, width), BF) for width in CUTS]

    return pl.pallas_call(
        whole_kernel,
        out_shape=(
            jax.ShapeDtypeStruct((TOK, D), BF),
            jax.ShapeDtypeStruct((LINES, WIDTH), BF),
        ),
        in_specs=[pl.BlockSpec(memory_space=pl.ANY)] * 3,
        out_specs=(pl.BlockSpec(memory_space=pl.ANY),) * 2,
        scratch_shapes=[
            pltpu.VMEM((TOK, D), BF),
            pltpu.VMEM((LINES, WIDTH), BF),
            pltpu.VMEM((1, TOK), jnp.int32),
            pltpu.VMEM((FEATS, TOK), BF),
            pltpu.VMEM((LINES, WIDTH), BF),
            pltpu.VMEM((GROUPS, 1, 2 * TOK), F32),
            pltpu.VMEM((GROUPS, 2 * TOK), F32),
            pltpu.VMEM((GROUPS, TOK), F32),
            pltpu.VMEM((GROUPS, TOK), F32),
            pltpu.VMEM((1, 2 * TOK), F32),
            pltpu.VMEM((YC, 16, FEATS), BF),
            pltpu.VMEM((YC, 16, FEATS), BF),
            pltpu.VMEM((4, FEATS, WIDTH), BF),
            pltpu.VMEM((2, 16, WIDTH), BF),
            pltpu.VMEM((TOK, TOK), BF),
            pltpu.VMEM((512, LINES), BF),
            pltpu.VMEM((1, 512), F32),
            pltpu.VMEM((ZL, 16, WIDTH), BF),
            pltpu.VMEM((GROUPS, 16, WIDTH), BF),
            pltpu.VMEM((GROUPS, 16, WIDTH), BF),
            *each(GROUPS, 16),
            *each(GROUPS, 16),
            *each(ZL, 16),
            *each(Z, 16),
            *each(4, 16),
            *each(YC, 4, 16),
            *each(8),
            dma((3,)), dma, dma, dma, dma, dma((8,)), dma, dma, dma, *[dma((N,))] * 9, dma,
        ],
        compiler_params=pltpu.CompilerParams(
            collective_id=0, has_side_effects=True, vmem_limit_bytes=60_000_000
        ),
        name="whole",
    )(token_ids.reshape(1, TOK), table, out_grad.T)


def solution(mesh):
    return jax.shard_map(
        body,
        mesh=mesh,
        in_specs=(P("dp"), P("segment", "dp"), P("dp", "segment")),
        out_specs=(P("dp", None), P("segment", "dp")),
        check_vma=False,
    )
```

```python
import jax
import jax.numpy as jnp
from jax import lax
from jax.experimental import pallas as pl
from jax.experimental.pallas import tpu as pltpu
from jax.sharding import PartitionSpec as P

MESH = pl.DeviceIdType.MESH
D = 3584
PACK = 8
TOK = 128
GROUPS = 32
X, ZL, ZH, YC = 4, 8, 2, 8
Z = ZH * ZL
LINES = 1188
WIDTH = 896
FEATS = 224
BF = jnp.bfloat16
F32 = jnp.float32
CUTS = (256, 384, 256)
STARTS = (0, 256, 640)
N = len(CUTS)


def coords():
    s = lax.axis_index("segment")
    d = lax.axis_index("dp")
    zh = s // YC
    k = s % YC
    x = d // ZL
    zl = d % ZL
    return zh, k, x, zl


def device(z, k, x):
    return ((z // ZL) * YC + k, x * ZL + z % ZL)


def plane_steps():
    return [(dx, dk) for dx in range(X) for dk in range(YC) if dx or dk]


def onehot(condition):
    return jnp.where(condition, F32(1), F32(0)).astype(BF)


def dot(a, b):
    return jnp.dot(a, b, preferred_element_type=F32).astype(BF)


def iota(shape, dim):
    return lax.broadcasted_iota(jnp.int32, shape, dim).astype(F32)


def remote(src, dst, send, recv, to):
    copy = pltpu.make_async_remote_copy(
        src_ref=src, dst_ref=dst, send_sem=send, recv_sem=recv, device_id=to, device_id_type=MESH
    )
    copy.start()
    return copy


def local(src, dst, sem):
    copy = pltpu.make_async_copy(src, dst, sem)
    copy.start()
    return copy


def settle(ref, sem):
    pltpu.make_async_copy(ref, ref, sem).wait()


def whole_kernel(
    ids_hbm, table_hbm, gradt_hbm, emb_ref, tg_ref,
    ids_ref, gradt_ref, table, info, flat, rt_ref, val_ref, mine, piece, got, place_at, gq, order_ref,
    s_ref, lrow_ref, dr, gs, gr, *rest,
):
    es, er, de, zr, fs, fr = (rest[n * N : (n + 1) * N] for n in range(6))
    (
        in_sem, id_send, id_recv, ft_send, ft_recv, zt_send, zt_recv, bt_send, bt_recv,
        ab_send, ab_recv, z_send, z_recv, f_send, f_recv, zt_pass,
    ) = rest[6 * N :]
    zh, k, x, zl = coords()
    z = zh * ZL + zl
    me = x * YC + k
    group = x * ZL + zl
    parity = zl // 4
    plane = plane_steps()
    near = [(dx, dz) for dx in range(X) for dz in range(-4, 5) if dz]

    barrier = pltpu.get_barrier_semaphore()
    for dx, dz in near:
        to = device((z + dz + Z) % Z, k, (x + dx) % X)
        pl.semaphore_signal(barrier, inc=1, device_id=to, device_id_type=MESH)
    for dx, dk in plane:
        to = device(z, (k + dk) % YC, (x + dx) % X)
        pl.semaphore_signal(barrier, inc=1, device_id=to, device_id_type=MESH)
    ids_copy = local(ids_hbm, ids_ref, in_sem.at[0])
    grad_copy = local(gradt_hbm, gradt_ref, in_sem.at[1])
    table_copy = local(table_hbm, table, in_sem.at[2])

    ids_copy.wait()
    ids = ids_ref[...]
    segment = ((ids.astype(F32) + 0.5) * F32(1.0 / (LINES * PACK))).astype(jnp.int32)
    slot = ids & 7
    key = ((segment * PACK + slot) * TOK + lax.broadcasted_iota(jnp.int32, (1, TOK), 1)).astype(F32)
    keys = jnp.broadcast_to(key, (TOK, TOK))
    at = jnp.sum(jnp.where(keys.T < keys, F32(1), F32(0)), axis=0, keepdims=True)
    mine[:, :TOK] = ids.astype(F32)
    mine[:, TOK:] = at
    at = at.astype(jnp.int32)
    klass, inside = at & 7, at >> 3
    order = jnp.where(
        iota((TOK, TOK), 0) == (klass * 16 + inside).astype(F32), F32(1), F32(0)
    )
    order_ref[...] = order.T.astype(BF)
    grad_copy.wait()
    sorted_grad = lax.dot_general(
        order.astype(BF), gradt_ref[...], (((1,), (1,)), ((), ())), preferred_element_type=F32
    ).astype(BF)
    piece[...] = sorted_grad.reshape(YC, 16, FEATS)
    for j in range(4):
        place_at[j] = onehot(iota((FEATS, WIDTH), 0) + F32(FEATS * j) == iota((FEATS, WIDTH), 1))

    pl.semaphore_wait(barrier, len(near) + len(plane))

    for dx, dz in [(dx, dz) for dx in range(X) for dz in range(-3, 5) if dx or dz]:
        remote(mine, info.at[group], id_send, id_recv, device((z + dz + Z) % Z, k, (x + dx) % X))
    local(mine, info.at[group], id_recv)
    for dk in range(1, YC):
        other = (k + dk) % YC
        remote(piece.at[other], got.at[k], ft_send, ft_recv, device(z, other, x))
    local(piece.at[k], got.at[k], ft_recv)

    settle(got, ft_recv)
    for h in range(2):
        total = jnp.zeros((16, WIDTH), F32)
        for j in range(4):
            total = total + jnp.dot(got[4 * h + j], place_at[j], preferred_element_type=F32)
        gq[h] = total.astype(BF)
    zt = []
    for h in range(2):
        ahead = (2 * zh + h + 4 - zl % 4) % 4
        up = pltpu.make_async_remote_copy(
            src_ref=gq.at[h],
            dst_ref=dr.at[zl],
            send_sem=zt_send.at[h],
            recv_sem=zt_recv.at[zl],
            device_id=device((z + ahead) % Z, k, x),
            device_id_type=MESH,
        )
        zt.append((ahead, up))

        @pl.when(ahead != 0)
        def _():
            up.start()

        @pl.when(ahead == 0)
        def _():
            local(gq.at[h], dr.at[zl], zt_recv.at[zl])

        remote(gq.at[h], dr.at[zl], zt_send.at[2 + h], zt_recv.at[zl], device((z + ahead + 12) % Z, k, x))

    settle(info, id_recv)
    for g in range(GROUPS):
        flat[g : g + 1, :] = info[g]
    ids = flat[:, :TOK]
    segment = ((ids + 0.5) * F32(1.0 / (LINES * PACK))).astype(jnp.int32)
    ids = ids.astype(jnp.int32)
    slot = ids & 7
    line = (ids - segment * (LINES * PACK)) >> 3
    at = flat[:, TOK:].astype(jnp.int32)
    klass, inside = at & 7, at >> 3
    second = inside & 1
    zg_row = lax.broadcasted_iota(jnp.int32, (GROUPS, TOK), 0) & 7
    my_bucket = (zh * YC + k) * PACK + 2 * x + parity
    code = jnp.where(segment * PACK + slot == my_bucket, klass * 16 + second + 2 * zg_row, -1).astype(F32)
    line = (line + 1).astype(F32)
    here = (klass == k) & (segment >> 3 == zh) & (slot & 1 == parity)
    rt_ref[...] = jnp.where(here, inside + 16 * zg_row, -1).astype(F32)
    source = ((slot >> 1) * YC + (segment & 7)) * 16 + second
    val_ref[...] = (source + 2 * zg_row + 1).astype(F32)

    sub = iota((TOK, TOK), 0)
    for ox in range(X):
        acc = jnp.zeros((TOK, TOK), F32)
        for g in range(ox * ZL, (ox + 1) * ZL):
            acc = acc + jnp.where(sub == code[g : g + 1], line[g : g + 1], F32(0))
        lcol = jnp.sum(acc, axis=1, keepdims=True) - 1
        lrow_ref[:, ox * TOK : (ox + 1) * TOK] = jnp.sum(acc.T, axis=0, keepdims=True) - 1
        s_ref[ox * TOK : (ox + 1) * TOK, :] = onehot(lcol == iota((TOK, LINES), 1))
    table_copy.wait()

    def plane_copies(src, dst, send, recv):
        for dx, dk in plane:
            ox, ok = (x + dx) % X, (k + dk) % YC
            remote(src.at[ox * YC + ok], dst.at[me], send, recv, device(z, ok, ox))
        local(src.at[me], dst.at[me], recv)

    past = [(z + Z - zl % 4 // 2 * ZL - zg) % Z for zg in range(ZL)]

    def pass_gradients():
        for zg, d in enumerate(past):
            @pl.when(d < 4)
            def _():
                settle(dr.at[zg], zt_recv.at[zg])
                remote(dr.at[zg], dr.at[zg], zt_pass.at[zg], zt_recv.at[zg], device((z + 4) % Z, k, x))

            @pl.when(d >= 12)
            def _():
                settle(dr.at[zg], zt_recv.at[zg])
                remote(dr.at[zg], dr.at[zg], zt_pass.at[zg], zt_recv.at[zg], device((z + 12) % Z, k, x))

    for c, (start, width) in enumerate(zip(STARTS, CUTS)):
        def pick_rows(i, carry):
            rows = pl.ds(pl.multiple_of(i * TOK, TOK), TOK)
            picked = dot(s_ref[rows, :], table[:, start : start + width])
            es[c][pl.ds(i * 8, 8)] = picked.reshape(8, 16, width)
            return carry

        lax.fori_loop(0, 4, pick_rows, 0)
        plane_copies(es[c], er[c], ab_send.at[c], ab_recv.at[c])
        if c == 0:
            pass_gradients()

    acc = jnp.zeros((TOK, TOK), F32)
    own = pl.ds(pl.multiple_of(x * ZL, ZL), ZL)
    rt, val = rt_ref[own, :], val_ref[own, :]
    for zg in range(ZL):
        acc = acc + jnp.where(sub == rt[zg : zg + 1], val[zg : zg + 1], F32(0))
    mcol = jnp.sum(acc, axis=1, keepdims=True) - 1
    mrow = jnp.sum(acc.T, axis=0, keepdims=True) - 1
    merge = onehot(mcol == iota((TOK, 512), 1))
    spread = onehot(iota((512, TOK), 0) == mrow)

    def merge_and_send(c):
        settle(er[c], ab_recv.at[c])
        de[c][...] = dot(merge, er[c][...].reshape(512, CUTS[c])).reshape(ZL, 16, CUTS[c])
        opposite = (z + 8) % Z
        remote(de[c].at[opposite % ZL], zr[c].at[z], z_send.at[c], z_recv.at[c], device(opposite, k, x))
        for dz in (9, 7, 10, 6, 11, 5, 12, 4, 13, 3, 14, 2, 15, 1):
            there = (z + dz) % Z
            remote(de[c].at[there % ZL], zr[c].at[z], z_send.at[c], z_recv.at[c], device(there, k, x))
        local(de[c].at[zl], zr[c].at[z], z_recv.at[c])

    merge_and_send(0)
    for zg, d in enumerate(past):
        @pl.when((d >= 4) & (d < 12))
        def _():
            settle(dr.at[zg], zt_recv.at[zg])
    gs[...] = dot(spread, dr[...].reshape(TOK, WIDTH)).reshape(GROUPS, 16, WIDTH)
    merge_and_send(1)
    plane_copies(gs, gr, bt_send, bt_recv)
    for c in range(2, N):
        merge_and_send(c)

    def sum_and_send(c):
        settle(zr[c], z_recv.at[c])
        for quarter in range(4):
            total = zr[c][quarter].astype(F32)
            for m in range(1, 4):
                total = total + zr[c][quarter + 4 * m].astype(F32)
            fs[c][quarter] = total.astype(BF)
        for dk in range(1, YC):
            remote(fs[c], fr[c].at[k], f_send.at[c], f_recv.at[c], device(z, (k + dk) % YC, x))
        local(fs[c], fr[c].at[k], f_recv.at[c])

    def finish(c):
        settle(fr[c], f_recv.at[c])
        for quarter in range(4):
            start = quarter * WIDTH + STARTS[c]
            rows = fr[c][:, quarter].reshape(TOK, CUTS[c])
            columns = slice(start, start + CUTS[c])
            emb_ref[:, columns] = dot(order_ref[...], rows)

    def scatter(start, rows):
        line = (start + lax.broadcasted_iota(jnp.int32, (rows, 512), 0)).astype(F32)
        place = onehot(line == lrow_ref[...])
        tg_ref[pl.ds(start, rows), :] = dot(place, gr[...].reshape(512, WIDTH))

    def scatter_step(i, carry):
        scatter(pl.multiple_of(i * TOK, TOK), TOK)
        return carry

    sum_and_send(0)
    sum_and_send(1)
    for c in range(2, N):
        finish(c - 2)
        sum_and_send(c)
    settle(gr, bt_recv)
    lax.fori_loop(0, LINES // TOK, scatter_step, 0)
    scatter(LINES // TOK * TOK, LINES % TOK)
    finish(N - 2)
    finish(N - 1)

    settle(info.at[pl.ds(0, GROUPS - 1)], id_send)
    settle(got.at[pl.ds(0, YC - 1)], ft_send)
    settle(gr.at[pl.ds(0, GROUPS - 1)], bt_send)
    for c in range(N):
        settle(er[c].at[pl.ds(0, GROUPS - 1)], ab_send.at[c])
        settle(zr[c].at[pl.ds(0, Z - 1)], z_send.at[c])
        settle(fr[c].at[pl.ds(0, YC - 1)], f_send.at[c])
    for h, (ahead, up) in enumerate(zt):
        settle(gq.at[h], zt_send.at[2 + h])

        @pl.when(ahead != 0)
        def _():
            up.wait_send()

    for zg, d in enumerate(past):
        @pl.when((d < 4) | (d >= 12))
        def _():
            settle(dr.at[zg], zt_pass.at[zg])


def body(token_ids, table, out_grad):
    dma = pltpu.SemaphoreType.DMA

    def each(*lead):
        return [pltpu.VMEM((*lead, width), BF) for width in CUTS]

    return pl.pallas_call(
        whole_kernel,
        out_shape=(
            jax.ShapeDtypeStruct((TOK, D), BF),
            jax.ShapeDtypeStruct((LINES, WIDTH), BF),
        ),
        in_specs=[pl.BlockSpec(memory_space=pl.ANY)] * 3,
        out_specs=(pl.BlockSpec(memory_space=pltpu.VMEM),) * 2,
        scratch_shapes=[
            pltpu.VMEM((1, TOK), jnp.int32),
            pltpu.VMEM((FEATS, TOK), BF),
            pltpu.VMEM((LINES, WIDTH), BF),
            pltpu.VMEM((GROUPS, 1, 2 * TOK), F32),
            pltpu.VMEM((GROUPS, 2 * TOK), F32),
            pltpu.VMEM((GROUPS, TOK), F32),
            pltpu.VMEM((GROUPS, TOK), F32),
            pltpu.VMEM((1, 2 * TOK), F32),
            pltpu.VMEM((YC, 16, FEATS), BF),
            pltpu.VMEM((YC, 16, FEATS), BF),
            pltpu.VMEM((4, FEATS, WIDTH), BF),
            pltpu.VMEM((2, 16, WIDTH), BF),
            pltpu.VMEM((TOK, TOK), BF),
            pltpu.VMEM((512, LINES), BF),
            pltpu.VMEM((1, 512), F32),
            pltpu.VMEM((ZL, 16, WIDTH), BF),
            pltpu.VMEM((GROUPS, 16, WIDTH), BF),
            pltpu.VMEM((GROUPS, 16, WIDTH), BF),
            *each(GROUPS, 16),
            *each(GROUPS, 16),
            *each(ZL, 16),
            *each(Z, 16),
            *each(4, 16),
            *each(YC, 4, 16),
            dma((3,)), dma, dma, dma, dma, dma((4,)), dma((8,)), dma, dma, *[dma((N,))] * 6, dma((8,)),
        ],
        compiler_params=pltpu.CompilerParams(
            collective_id=0, has_side_effects=True, vmem_limit_bytes=52_500_000
        ),
        name="whole",
    )(token_ids.reshape(1, TOK), table, out_grad.T)


def solution(mesh):
    return jax.shard_map(
        body,
        mesh=mesh,
        in_specs=(P("dp"), P("segment", "dp"), P("dp", "segment")),
        out_specs=(P("dp", None), P("segment", "dp")),
        check_vma=False,
    )
```

```python
import jax
import jax.numpy as jnp
from jax import lax
from jax.experimental import pallas as pl
from jax.experimental.pallas import tpu as pltpu
from jax.sharding import PartitionSpec as P

MESH = pl.DeviceIdType.MESH
D = 3584
PACK = 8
TOK = 128
GROUPS = 32
X, ZL, ZH, YC = 4, 8, 2, 8
Z = ZH * ZL
LINES = 1188
WIDTH = 896
FEATS = 224
BF = jnp.bfloat16
F32 = jnp.float32
CUTS = (256, 384, 256)
STARTS = (0, 256, 640)
N = len(CUTS)


def coords():
    s = lax.axis_index("segment")
    d = lax.axis_index("dp")
    zh = s // YC
    k = s % YC
    x = d // ZL
    zl = d % ZL
    return zh, k, x, zl


def device(z, k, x):
    return ((z // ZL) * YC + k, x * ZL + z % ZL)


def plane_steps():
    return [(dx, dk) for dx in range(X) for dk in range(YC) if dx or dk]


def onehot(condition):
    return jnp.where(condition, F32(1), F32(0)).astype(BF)


def dot(a, b):
    return jnp.dot(a, b, preferred_element_type=F32).astype(BF)


def iota(shape, dim):
    return lax.broadcasted_iota(jnp.int32, shape, dim).astype(F32)


def remote(src, dst, send, recv, to):
    copy = pltpu.make_async_remote_copy(
        src_ref=src, dst_ref=dst, send_sem=send, recv_sem=recv, device_id=to, device_id_type=MESH
    )
    copy.start()
    return copy


def local(src, dst, sem):
    copy = pltpu.make_async_copy(src, dst, sem)
    copy.start()
    return copy


def settle(ref, sem):
    pltpu.make_async_copy(ref, ref, sem).wait()


def whole_kernel(
    ids_hbm, table_hbm, gradt_hbm, emb_ref, tg_ref,
    ids_ref, gradt_ref, table, info, flat, code_ref, line_ref, found_ref, rt_ref, val_ref, mine, piece, got, gq, order_ref,
    s_ref, lrow_ref, dr, gs, gr, *rest,
):
    es, er, de, zr, fs, fr = (rest[n * N : (n + 1) * N] for n in range(6))
    (
        in_sem, id_send, id_recv, ft_send, ft_recv, zt_send, zt_recv, bt_send, bt_recv,
        ab_send, ab_recv, z_send, z_recv, f_send, f_recv, zt_pass,
    ) = rest[6 * N :]
    zh, k, x, zl = coords()
    z = zh * ZL + zl
    me = x * YC + k
    group = x * ZL + zl
    parity = zl // 4
    plane = plane_steps()
    near = [(dx, dz) for dx in range(X) for dz in range(-4, 5) if dz]

    barrier = pltpu.get_barrier_semaphore()
    for dx, dz in near:
        to = device((z + dz + Z) % Z, k, (x + dx) % X)
        pl.semaphore_signal(barrier, inc=1, device_id=to, device_id_type=MESH)
    for dx, dk in plane:
        to = device(z, (k + dk) % YC, (x + dx) % X)
        pl.semaphore_signal(barrier, inc=1, device_id=to, device_id_type=MESH)
    ids_copy = local(ids_hbm, ids_ref, in_sem.at[0])
    grad_copy = local(gradt_hbm, gradt_ref, in_sem.at[1])
    table_copy = local(table_hbm, table, in_sem.at[2])

    ids_copy.wait()
    ids = ids_ref[...]
    segment = ((ids.astype(F32) + 0.5) * F32(1.0 / (LINES * PACK))).astype(jnp.int32)
    slot = ids & 7
    key = ((segment * PACK + slot) * TOK + lax.broadcasted_iota(jnp.int32, (1, TOK), 1)).astype(F32)
    keys = jnp.broadcast_to(key, (TOK, TOK))
    at = jnp.sum(jnp.where(keys.T < keys, F32(1), F32(0)), axis=0, keepdims=True)
    mine[:, :TOK] = ids.astype(F32)
    mine[:, TOK:] = at
    at = at.astype(jnp.int32)
    klass, inside = at & 7, at >> 3
    order = jnp.where(
        iota((TOK, TOK), 0) == (klass * 16 + inside).astype(F32), F32(1), F32(0)
    )
    order_ref[...] = order.T.astype(BF)
    grad_copy.wait()
    sorted_grad = lax.dot_general(
        order.astype(BF), gradt_ref[...], (((1,), (1,)), ((), ())), preferred_element_type=F32
    ).astype(BF)
    piece[...] = sorted_grad.reshape(YC, 16, FEATS)
    pl.semaphore_wait(barrier, len(near) + len(plane))

    for dx, dz in [(dx, dz) for dx in range(X) for dz in range(-3, 5) if dx or dz]:
        remote(mine, info.at[group], id_send, id_recv, device((z + dz + Z) % Z, k, (x + dx) % X))
    local(mine, info.at[group], id_recv)
    for dk in range(1, YC):
        other = (k + dk) % YC
        remote(piece.at[other], got.at[k], ft_send, ft_recv, device(z, other, x))
    local(piece.at[k], got.at[k], ft_recv)

    settle(got, ft_recv)
    for h in range(2):
        quarters = [got[4 * h + j].astype(F32) for j in range(4)]
        gq[h] = jnp.concatenate(quarters, axis=1).astype(BF)
    zt = []
    for h in range(2):
        ahead = (2 * zh + h + 4 - zl % 4) % 4
        up = pltpu.make_async_remote_copy(
            src_ref=gq.at[h],
            dst_ref=dr.at[zl],
            send_sem=zt_send.at[h],
            recv_sem=zt_recv.at[zl],
            device_id=device((z + ahead) % Z, k, x),
            device_id_type=MESH,
        )
        zt.append((ahead, up))

        @pl.when(ahead != 0)
        def _():
            up.start()

        @pl.when(ahead == 0)
        def _():
            local(gq.at[h], dr.at[zl], zt_recv.at[zl])

        remote(gq.at[h], dr.at[zl], zt_send.at[2 + h], zt_recv.at[zl], device((z + ahead + 12) % Z, k, x))

    settle(info, id_recv)
    for g in range(GROUPS):
        flat[g : g + 1, :] = info[g]
    ids = flat[:, :TOK]
    segment = ((ids + 0.5) * F32(1.0 / (LINES * PACK))).astype(jnp.int32)
    ids = ids.astype(jnp.int32)
    slot = ids & 7
    line = (ids - segment * (LINES * PACK)) >> 3
    at = flat[:, TOK:].astype(jnp.int32)
    klass, inside = at & 7, at >> 3
    second = inside & 1
    zg_row = lax.broadcasted_iota(jnp.int32, (GROUPS, TOK), 0) & 7
    my_bucket = (zh * YC + k) * PACK + 2 * x + parity
    code = jnp.where(segment * PACK + slot == my_bucket, klass * 16 + second + 2 * zg_row, -1).astype(F32)
    line = (line + 1).astype(F32)
    here = (klass == k) & (segment >> 3 == zh) & (slot & 1 == parity)
    rt_ref[...] = jnp.where(here, inside + 16 * zg_row, -1).astype(F32)
    source = ((slot >> 1) * YC + (segment & 7)) * 16 + second
    val_ref[...] = (source + 2 * zg_row + 1).astype(F32)

    code_ref[...] = code
    line_ref[...] = line

    sub = iota((TOK, TOK), 0)
    table_copy.wait()
    for dx in range(X):
        ox = (x + dx) % X
        groups = pl.ds(pl.multiple_of(ox * ZL, ZL), ZL)
        codes, lines = code_ref[groups, :], line_ref[groups, :]
        acc = jnp.zeros((TOK, TOK), F32)
        for zg in range(ZL):
            acc = acc + jnp.where(sub == codes[zg : zg + 1], lines[zg : zg + 1], F32(0))
        found_ref[ox] = acc
        lcol = jnp.sum(acc, axis=1, keepdims=True) - 1
        pick = onehot(lcol == iota((TOK, LINES), 1))
        s_ref[pl.ds(pl.multiple_of(ox * TOK, TOK), TOK), :] = pick
        es[0][pl.ds(ox * YC, YC)] = dot(pick, table[:, : CUTS[0]]).reshape(YC, 16, CUTS[0])
        for dk in range(YC):
            ok = (k + dk) % YC
            if dx or dk:
                remote(es[0].at[ox * YC + ok], er[0].at[me], ab_send.at[0], ab_recv.at[0], device(z, ok, ox))
            else:
                local(es[0].at[me], er[0].at[me], ab_recv.at[0])

    def plane_copies(src, dst, send, recv):
        for dx, dk in plane:
            ox, ok = (x + dx) % X, (k + dk) % YC
            remote(src.at[ox * YC + ok], dst.at[me], send, recv, device(z, ok, ox))
        local(src.at[me], dst.at[me], recv)

    past = [(z + Z - zl % 4 // 2 * ZL - zg) % Z for zg in range(ZL)]

    def pass_gradients():
        for zg, d in enumerate(past):
            @pl.when(d < 4)
            def _():
                settle(dr.at[zg], zt_recv.at[zg])
                remote(dr.at[zg], dr.at[zg], zt_pass.at[zg], zt_recv.at[zg], device((z + 4) % Z, k, x))

            @pl.when(d >= 12)
            def _():
                settle(dr.at[zg], zt_recv.at[zg])
                remote(dr.at[zg], dr.at[zg], zt_pass.at[zg], zt_recv.at[zg], device((z + 12) % Z, k, x))

    pass_gradients()
    for c in range(1, N):
        def pick_rows(i, carry):
            rows = pl.ds(pl.multiple_of(i * TOK, TOK), TOK)
            picked = dot(s_ref[rows, :], table[:, STARTS[c] : STARTS[c] + CUTS[c]])
            es[c][pl.ds(i * 8, 8)] = picked.reshape(8, 16, CUTS[c])
            return carry

        lax.fori_loop(0, 4, pick_rows, 0)
        plane_copies(es[c], er[c], ab_send.at[c], ab_recv.at[c])

    acc = jnp.zeros((TOK, TOK), F32)
    own = pl.ds(pl.multiple_of(x * ZL, ZL), ZL)
    rt, val = rt_ref[own, :], val_ref[own, :]
    for zg in range(ZL):
        acc = acc + jnp.where(sub == rt[zg : zg + 1], val[zg : zg + 1], F32(0))
    mcol = jnp.sum(acc, axis=1, keepdims=True) - 1
    mrow = jnp.sum(acc.T, axis=0, keepdims=True) - 1
    merge = onehot(mcol == iota((TOK, 512), 1))
    spread = onehot(iota((512, TOK), 0) == mrow)

    def merge_and_send(c):
        settle(er[c], ab_recv.at[c])
        de[c][...] = dot(merge, er[c][...].reshape(512, CUTS[c])).reshape(ZL, 16, CUTS[c])
        opposite = (z + 8) % Z
        remote(de[c].at[opposite % ZL], zr[c].at[z], z_send.at[c], z_recv.at[c], device(opposite, k, x))
        for dz in (9, 7, 10, 6, 11, 5, 12, 4, 13, 3, 14, 2, 15, 1):
            there = (z + dz) % Z
            remote(de[c].at[there % ZL], zr[c].at[z], z_send.at[c], z_recv.at[c], device(there, k, x))
        local(de[c].at[zl], zr[c].at[z], z_recv.at[c])

    merge_and_send(0)
    for zg, d in enumerate(past):
        @pl.when((d >= 4) & (d < 12))
        def _():
            settle(dr.at[zg], zt_recv.at[zg])
    gs[...] = dot(spread, dr[...].reshape(TOK, WIDTH)).reshape(GROUPS, 16, WIDTH)
    merge_and_send(1)
    plane_copies(gs, gr, bt_send, bt_recv)
    for c in range(2, N):
        merge_and_send(c)

    def sum_and_send(c):
        settle(zr[c], z_recv.at[c])
        for quarter in range(4):
            total = zr[c][quarter].astype(F32)
            for m in range(1, 4):
                total = total + zr[c][quarter + 4 * m].astype(F32)
            fs[c][quarter] = total.astype(BF)
        for dk in range(1, YC):
            remote(fs[c], fr[c].at[k], f_send.at[c], f_recv.at[c], device(z, (k + dk) % YC, x))
        local(fs[c], fr[c].at[k], f_recv.at[c])

    def finish(c):
        settle(fr[c], f_recv.at[c])
        for quarter in range(4):
            start = quarter * WIDTH + STARTS[c]
            rows = fr[c][:, quarter].reshape(TOK, CUTS[c])
            columns = slice(start, start + CUTS[c])
            emb_ref[:, columns] = dot(order_ref[...], rows)

    def scatter(start, rows):
        line = (start + lax.broadcasted_iota(jnp.int32, (rows, 512), 0)).astype(F32)
        place = onehot(line == lrow_ref[...])
        tg_ref[pl.ds(start, rows), :] = dot(place, gr[...].reshape(512, WIDTH))

    def scatter_step(i, carry):
        scatter(pl.multiple_of(i * TOK, TOK), TOK)
        return carry

    sum_and_send(0)
    sum_and_send(1)
    for c in range(2, N):
        finish(c - 2)
        sum_and_send(c)
    for ox in range(X):
        lrow_ref[:, ox * TOK : (ox + 1) * TOK] = jnp.sum(found_ref[ox].T, axis=0, keepdims=True) - 1
    settle(gr, bt_recv)
    lax.fori_loop(0, LINES // TOK, scatter_step, 0)
    scatter(LINES // TOK * TOK, LINES % TOK)
    finish(N - 2)
    finish(N - 1)

    settle(info.at[pl.ds(0, GROUPS - 1)], id_send)
    settle(got.at[pl.ds(0, YC - 1)], ft_send)
    settle(gr.at[pl.ds(0, GROUPS - 1)], bt_send)
    for c in range(N):
        settle(er[c].at[pl.ds(0, GROUPS - 1)], ab_send.at[c])
        settle(zr[c].at[pl.ds(0, Z - 1)], z_send.at[c])
        settle(fr[c].at[pl.ds(0, YC - 1)], f_send.at[c])
    for h, (ahead, up) in enumerate(zt):
        settle(gq.at[h], zt_send.at[2 + h])

        @pl.when(ahead != 0)
        def _():
            up.wait_send()

    for zg, d in enumerate(past):
        @pl.when((d < 4) | (d >= 12))
        def _():
            settle(dr.at[zg], zt_pass.at[zg])


def body(token_ids, table, out_grad):
    dma = pltpu.SemaphoreType.DMA

    def each(*lead):
        return [pltpu.VMEM((*lead, width), BF) for width in CUTS]

    return pl.pallas_call(
        whole_kernel,
        out_shape=(
            jax.ShapeDtypeStruct((TOK, D), BF),
            jax.ShapeDtypeStruct((LINES, WIDTH), BF),
        ),
        in_specs=[pl.BlockSpec(memory_space=pl.ANY)] * 3,
        out_specs=(pl.BlockSpec(memory_space=pltpu.VMEM),) * 2,
        scratch_shapes=[
            pltpu.VMEM((1, TOK), jnp.int32),
            pltpu.VMEM((FEATS, TOK), BF),
            pltpu.VMEM((LINES, WIDTH), BF),
            pltpu.VMEM((GROUPS, 1, 2 * TOK), F32),
            pltpu.VMEM((GROUPS, 2 * TOK), F32),
            pltpu.VMEM((GROUPS, TOK), F32),
            pltpu.VMEM((GROUPS, TOK), F32),
            pltpu.VMEM((X, TOK, TOK), F32),
            pltpu.VMEM((GROUPS, TOK), F32),
            pltpu.VMEM((GROUPS, TOK), F32),
            pltpu.VMEM((1, 2 * TOK), F32),
            pltpu.VMEM((YC, 16, FEATS), BF),
            pltpu.VMEM((YC, 16, FEATS), BF),
            pltpu.VMEM((2, 16, WIDTH), BF),
            pltpu.VMEM((TOK, TOK), BF),
            pltpu.VMEM((512, LINES), BF),
            pltpu.VMEM((1, 512), F32),
            pltpu.VMEM((ZL, 16, WIDTH), BF),
            pltpu.VMEM((GROUPS, 16, WIDTH), BF),
            pltpu.VMEM((GROUPS, 16, WIDTH), BF),
            *each(GROUPS, 16),
            *each(GROUPS, 16),
            *each(ZL, 16),
            *each(Z, 16),
            *each(4, 16),
            *each(YC, 4, 16),
            dma((3,)), dma, dma, dma, dma, dma((4,)), dma((8,)), dma, dma, *[dma((N,))] * 6, dma((8,)),
        ],
        compiler_params=pltpu.CompilerParams(
            collective_id=0, has_side_effects=True, vmem_limit_bytes=52_500_000
        ),
        name="whole",
    )(token_ids.reshape(1, TOK), table, out_grad.T)


def solution(mesh):
    return jax.shard_map(
        body,
        mesh=mesh,
        in_specs=(P("dp"), P("segment", "dp"), P("dp", "segment")),
        out_specs=(P("dp", None), P("segment", "dp")),
        check_vma=False,
    )
```
